32 devices in a mesh: head: 8 (over z, y), ctx: 4 (over x, core).
Axes of the slice: x: 2, y: 2, z: 4, core: 2. Of those that a mesh axis runs over, the one named last changes fastest.
Arguments:
- query: bfloat16 [3072, 4096], P(('ctx', 'head')), may hold values from -8 to 8
- key: bfloat16 [3072, 2048], P(('ctx', 'head')), may hold values from -8 to 8
- value: bfloat16 [3072, 2048], P(('ctx', 'head')), may hold values from -8 to 8
- block_order: int32 [8], replicated, may hold values from 0 to 7, each once
Outputs:
- attended: bfloat16 [3072, 4096], P('ctx', 'head')
The draws below stay inside these ranges and needn't reach their ends.
Inputs may be any that keep to these rules, and one draw needn't show every extreme that they name: `block_order`: each storage block index 0 to 7 appears exactly once.
All inputs are finite; a program needn't handle non-finite values.
Results may differ from the reference program's by a relative error of at most 0.0049.
Values may be sent and summed in bfloat16 or wider, within the bound.
A program may use at most 128 MiB of HBM per device.

```python
import jax
import jax.numpy as jnp
from jax import lax

HQ = 32
KEY_HEADS = 16
HEAD_WIDTH = 128
QUERY_PER_KEY = 2
TOKEN_COUNT = 3072
BLK = 384
BLOCKS = 8


def levels(stream_key, dims, split, low, high):
    factor_of, own = 1.0, jax.random.fold_in(stream_key, 6)
    for position, shards_of in split:
        draws = jnp.exp(jax.random.uniform(jax.random.fold_in(own, position), (shards_of,), jnp.float32, low / len(split), high / len(split)))
        factor_of = factor_of * jnp.repeat(draws, dims[position] // shards_of).reshape([-1 if axis == position else 1 for axis in range(len(dims))])
    return factor_of


def scatter_about(stream_key, shape, spread, most, cuts=(), held_as=jnp.bfloat16):
    values = spread * jax.random.normal(stream_key, shape, jnp.float32)
    if cuts:
        values = values * levels(stream_key, shape, cuts, -0.22, 0.18)
    return jnp.clip(values, -most, most).astype(held_as)


def setup_inputs(seed: int = 0) -> dict:
    streams_of = jax.random.split(jax.random.key(seed), 5)
    query = scatter_about(streams_of[0], (TOKEN_COUNT, HQ * HEAD_WIDTH), 1.5, 8.0, ((0, 32),))
    key = scatter_about(streams_of[1], (TOKEN_COUNT, KEY_HEADS * HEAD_WIDTH), 1.0, 8.0, ((0, 32),))
    value = scatter_about(streams_of[2], (TOKEN_COUNT, KEY_HEADS * HEAD_WIDTH), 1.0, 8.0, ((0, 32),))
    block_order = jax.random.permutation(streams_of[3], BLOCKS).astype(jnp.int32)
    return {"query": query, "key": key, "value": value, "block_order": block_order}


query_scale = 1.0 / 12.0
softcap_limit = 50.0


def head_block(query_rows, key_rows, value_rows, query_pos, key_pos):
    scores = jnp.einsum('rgd,kd->grk', query_rows.astype(jnp.float32), key_rows.astype(jnp.float32)) * query_scale
    capped = softcap_limit * jnp.tanh(scores / softcap_limit)
    visible = key_pos[None, :] <= query_pos[:, None]
    weights = jnp.where(visible[None], jnp.exp(capped), jnp.zeros_like(capped))
    denominator = jnp.sum(weights, axis=-1)
    rounded = lax.optimization_barrier(weights.astype(jnp.bfloat16)).astype(jnp.float32)
    numerator = jnp.einsum('grk,kd->grd', rounded, value_rows.astype(jnp.float32))
    return jnp.transpose(numerator / denominator[..., None], (1, 0, 2))


def reference(query, key, value, block_order):
    sequence_length = query.shape[0]
    positions = (block_order[:, None].astype(jnp.int32) * BLK + jnp.arange(BLK, dtype=jnp.int32)[None, :]).reshape(sequence_length)
    row_block = 2 * BLK
    block_count = sequence_length // row_block
    query_rows = query.reshape(sequence_length, KEY_HEADS, QUERY_PER_KEY, HEAD_WIDTH)
    key_rows = key.reshape(sequence_length, KEY_HEADS, HEAD_WIDTH)
    value_rows = value.reshape(sequence_length, KEY_HEADS, HEAD_WIDTH)
    columns = []
    for key_value_head in range(KEY_HEADS):
        def one_block(pieces, key_value_head=key_value_head):
            return head_block(pieces[0], key_rows[:, key_value_head], value_rows[:, key_value_head], pieces[1], positions)
        blocks = lax.map(one_block, (query_rows[:, key_value_head].reshape(block_count, row_block, QUERY_PER_KEY, HEAD_WIDTH), positions.reshape(block_count, row_block)))
        columns.append(blocks.reshape(sequence_length, QUERY_PER_KEY * HEAD_WIDTH))
    return jnp.concatenate(columns, axis=1).astype(jnp.bfloat16)
```

```python
import functools
import math

import jax
import jax.numpy as jnp
from jax import lax
from jax.experimental import pallas as pl
from jax.experimental.pallas import tpu as pltpu
from jax.sharding import PartitionSpec as P

HEAD_WIDTH = 128
MESH = pl.DeviceIdType.MESH
CAP = 50.0
IN_SCALE = 1.0 / (12.0 * CAP)
OUT_SCALE = CAP * math.log2(math.e)
HIDDEN = -4096.0


def flip(index, step, size):
    out, bit = 0, 1
    while bit < size:
        mine = (index // bit) % 2
        turn = (step // bit) % 2
        out = out + (mine + turn - 2 * mine * turn) * bit
        bit *= 2
    return out


def kernel(
    n_head, n_ctx, pair,
    order, query, key, value, out,
    qbuf, kv, acc,
    q_send, k_send, v_send, q_recv, k_recv, v_recv,
    local_sem, x_send, p_send, f_recv,
):
    me = lax.axis_index("head")
    ctx = lax.axis_index("ctx")
    chip, core = ctx // 2, ctx % 2
    partner = chip * 2 + 1 - core
    chips = n_ctx // 2
    pieces = n_head // pair
    rows = query.shape[0]
    total = rows * n_head
    block = total // 2
    q_cols = query.shape[1] // n_head
    kv_cols = key.shape[1] // n_head
    kv_heads = kv_cols // HEAD_WIDTH
    per_kv = q_cols // kv_cols
    h_cols = per_kv * HEAD_WIDTH
    piece_rows = rows * pair
    near_pieces = pieces // 2
    near = n_head // 2
    home = me // pair
    near_half = home // near_pieces
    far_half = 1 - near_half
    inner = (home + home // near_pieces) % 2
    same_core = [((chip + t) % chips) * 2 + core for t in range(chips)]
    other_core = [((chip + t) % chips) * 2 + 1 - core for t in range(chips)]
    peers = [flip(me, j, n_head) for j in range(1, n_head)]

    barrier = pltpu.get_barrier_semaphore()
    for d in peers:
        pl.semaphore_signal(barrier, inc=1, device_id={"head": d}, device_id_type=MESH)
    for c in [partner] + same_core[1:]:
        pl.semaphore_signal(barrier, inc=1, device_id={"ctx": c}, device_id_type=MESH)
    def rows_of(s):
        return pl.ds(pl.multiple_of(s * rows, rows), rows)

    def cols_of(s, width):
        return pl.ds(pl.multiple_of(s * width, width), width)

    mine = [
        pltpu.make_async_copy(key.at[:, cols_of(me, kv_cols)], kv.at[ctx, 0, rows_of(me)], local_sem.at[0]),
        pltpu.make_async_copy(value.at[:, cols_of(me, kv_cols)], kv.at[ctx, 1, rows_of(me)], local_sem.at[1]),
        pltpu.make_async_copy(query.at[:, cols_of(me, q_cols)], qbuf.at[rows_of(me)], local_sem.at[2]),
    ]
    for copy in mine:
        copy.start()

    pl.semaphore_wait(barrier, n_head - 1 + chips)

    def kv_sends(d):
        return [
            pltpu.make_async_remote_copy(
                src_ref=src.at[:, cols_of(d, kv_cols)], dst_ref=kv.at[ctx, i, rows_of(me)],
                send_sem=send.at[d], recv_sem=recv.at[me],
                device_id={"head": d}, device_id_type=MESH,
            )
            for i, (src, send, recv) in enumerate(((key, k_send, k_recv), (value, v_send, v_recv)))
        ]

    def q_send_to(d, h):
        return pltpu.make_async_remote_copy(
            src_ref=query.at[:, cols_of(d * kv_heads + h, h_cols)],
            dst_ref=qbuf.at[rows_of(me), h * h_cols : (h + 1) * h_cols],
            send_sem=q_send.at[h, d], recv_sem=q_recv.at[h, me],
            device_id={"head": d}, device_id_type=MESH,
        )

    sends = [copy for d in peers[near - 1 :] for copy in kv_sends(d)]
    sends += [copy for d in peers[: near - 1] for copy in kv_sends(d)]
    sends += [q_send_to(d, h) for d in peers[: near - 1] for h in range(kv_heads)]
    turned = peers[near - 1 + near // 2 :] + peers[near - 1 : near - 1 + near // 2]
    sends += [q_send_to(d, h) for h in range(kv_heads) for d in turned]
    for copy in sends:
        copy.start()

    def arrived(ref, sem):
        pltpu.make_async_copy(ref, ref, sem).wait()

    def kv_ref(c, s):
        return kv.at[c, :, rows_of(s)]

    def pass_on(c, s, dest, send):
        copy = pltpu.make_async_remote_copy(
            src_ref=kv_ref(c, s), dst_ref=kv_ref(c, s),
            send_sem=send, recv_sem=f_recv.at[c, s],
            device_id={"ctx": dest}, device_id_type=MESH,
        )
        copy.start()

    def spread(j):
        s = flip(me, j, n_head)
        if isinstance(j, int) and j == 0:
            mine[0].wait()
            mine[1].wait()
        else:
            arrived(kv.at[ctx, 0, rows_of(s)], k_recv.at[s])
            arrived(kv.at[ctx, 1, rows_of(s)], v_recv.at[s])
        for c in same_core[1:]:
            pass_on(ctx, s, c, x_send.at[c, s])
        pass_on(ctx, s, partner, p_send.at[ctx, s])

    def relay(j):
        s = flip(me, j, n_head)
        for c in same_core[1:]:
            arrived(kv_ref(c, s), f_recv.at[c, s])
            pass_on(c, s, partner, p_send.at[c, s])

    def from_partner(j):
        s = flip(me, j, n_head)
        for c in other_core:
            arrived(kv_ref(c, s), f_recv.at[c, s])

    ones = jnp.ones((2 * block, HEAD_WIDTH), jnp.bfloat16)

    def unit(h, first_row, half, t, diagonal):
        q_half = first_row // block
        q_block = order[2 * ctx + q_half]
        c0 = ((chip + t) % chips) * 2 + core
        c1 = ((chip + t) % chips) * 2 + 1 - core
        q_span = pl.ds(pl.multiple_of(first_row, piece_rows), piece_rows)
        k_span = pl.ds(pl.multiple_of(half * block, block), block)
        low = jnp.where(order[2 * c0 + half] <= q_block, 0.0, HIDDEN)
        high = jnp.where(order[2 * c1 + half] <= q_block, 0.0, HIDDEN)
        cols = slice(h * HEAD_WIDTH, (h + 1) * HEAD_WIDTH)
        q = jnp.concatenate(
            [qbuf[q_span, (h * per_kv + i) * HEAD_WIDTH : (h * per_kv + i + 1) * HEAD_WIDTH] for i in range(per_kv)],
            axis=0,
        )
        k = jnp.concatenate([kv[c0, 0, k_span, cols], kv[c1, 0, k_span, cols]], axis=0)
        v = jnp.concatenate([kv[c0, 1, k_span, cols], kv[c1, 1, k_span, cols]], axis=0)
        x = lax.dot_general(q, k, (((1,), (1,)), ((), ())), preferred_element_type=jnp.float32)
        x = jnp.tanh(x * IN_SCALE) * OUT_SCALE
        if diagonal:
            q_at = first_row - q_half * block + lax.broadcasted_iota(jnp.int32, (piece_rows, block), 0)
            visible = lax.broadcasted_iota(jnp.int32, (piece_rows, block), 1) <= q_at
            e = jnp.exp2(x[:, :block]).reshape(per_kv, piece_rows, block)
            left = jnp.where(visible[None], e, 0.0).reshape(per_kv * piece_rows, block)
        else:
            left = jnp.exp2(x[:, :block] + low)
        w = jnp.concatenate([left, jnp.exp2(x[:, block:] + high)], axis=1).astype(jnp.bfloat16)
        return jnp.dot(w, jnp.concatenate([v, ones], axis=1), preferred_element_type=jnp.float32)

    def q_arrived(h, j):
        s = flip(me, j, n_head)
        arrived(qbuf.at[rows_of(s), h * h_cols : (h + 1) * h_cols], q_recv.at[h, s])

    def finish(h, first_row, at):
        span = pl.ds(pl.multiple_of(first_row, piece_rows), piece_rows)
        a = acc[at, h]
        o = (a[:, :HEAD_WIDTH] / a[:, HEAD_WIDTH:]).astype(jnp.bfloat16)
        for i in range(per_kv):
            col = (h * per_kv + i) * HEAD_WIDTH
            out[span, col : col + HEAD_WIDTH] = o[i * piece_rows : (i + 1) * piece_rows]

    def each(count, body):
        lax.fori_loop(0, count, lambda i, carry: (body(i), carry)[1], 0)

    near_steps = range(near_pieces)
    far_steps = [near_pieces + flip(1 - inner, k, near_pieces) for k in near_steps]

    def far_peers(k):
        return [far_steps[k] * pair + t for t in range(pair)]

    def near_near(step):
        for t in range(pair):
            j = step * pair + t
            if step + t == 0:
                mine[2].wait()
            else:
                for h in range(kv_heads):
                    q_arrived(h, j)
        first_row = flip(home, step, pieces) * piece_rows
        for h in range(kv_heads):
            acc[step, h] = unit(h, first_row, near_half, 0, True)

        def more(t):
            for h in range(kv_heads):
                acc[step, h] += unit(h, first_row, near_half, t + 1, False)

        each(chips - 1, more)

    for j in range(pair):
        spread(j)

    @pl.when(inner == 0)
    def _():
        for j in range(pair, near):
            spread(j)

    for j in far_peers(0):
        spread(j)

    @pl.when(inner == 1)
    def _():
        for j in range(pair, near):
            spread(j)

    for k in near_steps[1:]:
        for j in far_peers(k):
            spread(j)
    for j in range(near):
        relay(j)
    for j in range(near):
        from_partner(j)
    near_near(0)
    for j in far_peers(0):
        relay(j)
    for step in near_steps[1:]:
        near_near(step)
    for k in near_steps[1:]:
        for j in far_peers(k):
            relay(j)
    for k in near_steps:
        for j in far_peers(k):
            from_partner(j)

    def rest(step):
        first_row = flip(home, step, pieces) * piece_rows
        def more(t):
            for h in range(kv_heads):
                acc[step, h] += unit(h, first_row, far_half, t, False)

        each(chips, more)
        for h in range(kv_heads):
            finish(h, first_row, step)

    each(near_pieces, rest)

    for h in range(kv_heads):
        def far_all(k):
            step = near_pieces + flip(1 - inner, k, near_pieces)
            for t in range(pair):
                q_arrived(h, step * pair + t)
            first_row = flip(home, step, pieces) * piece_rows
            acc[near_pieces, h] = unit(h, first_row, far_half, 0, True) + unit(h, first_row, near_half, 0, False)

            def more(t):
                acc[near_pieces, h] += unit(h, first_row, far_half, t + 1, False) + unit(h, first_row, near_half, t + 1, False)

            each(chips - 1, more)
            finish(h, first_row, near_pieces)

        each(near_pieces, far_all)
    for copy in sends:
        copy.wait_send()
    for s in range(n_head):
        for c in same_core:
            arrived(kv_ref(c, s), p_send.at[c, s])
        for c in same_core[1:]:
            arrived(kv_ref(ctx, s), x_send.at[c, s])


def shards(n_head, n_ctx, query, key, value, block_order):
    rows = query.shape[0]
    total = rows * n_head
    q_cols = query.shape[1] // n_head
    kv_cols = key.shape[1] // n_head
    kv_heads = kv_cols // HEAD_WIDTH
    per_kv = q_cols // kv_cols
    pair = 2
    pieces = n_head // pair
    hbm = pl.BlockSpec(memory_space=pltpu.HBM)
    dma = pltpu.SemaphoreType.DMA
    return pl.pallas_call(
        functools.partial(kernel, n_head, n_ctx, pair),
        out_shape=jax.ShapeDtypeStruct((total, q_cols), jnp.bfloat16),
        in_specs=[pl.BlockSpec(memory_space=pltpu.SMEM), hbm, hbm, hbm],
        out_specs=pl.BlockSpec(memory_space=pltpu.VMEM),
        scratch_shapes=[
            pltpu.VMEM((total, q_cols), jnp.bfloat16),
            pltpu.VMEM((n_ctx, 2, total, kv_cols), jnp.bfloat16),
            pltpu.VMEM((pieces // 2 + 1, kv_heads, per_kv * pair * rows, 2 * HEAD_WIDTH), jnp.float32),
            dma((kv_heads, n_head)), dma((n_head,)), dma((n_head,)),
            dma((kv_heads, n_head)), dma((n_head,)), dma((n_head,)),
            dma((3,)),
            dma((n_ctx, n_head)), dma((n_ctx, n_head)), dma((n_ctx, n_head)),
        ],
        compiler_params=pltpu.CompilerParams(
            collective_id=0, has_side_effects=True, vmem_limit_bytes=60 * 1024 * 1024
        ),
    )(block_order, query, key, value)


def solution(mesh):
    placed = (P(("ctx", "head"), None), P(("ctx", "head"), None), P(("ctx", "head"), None), P())
    return jax.shard_map(
        functools.partial(shards, mesh.shape["head"], mesh.shape["ctx"]),
        mesh=mesh, in_specs=placed, out_specs=P("ctx", "head"), check_vma=False,
    )
```

```python
import functools
import math

import jax
import jax.numpy as jnp
from jax import lax
from jax.experimental import pallas as pl
from jax.experimental.pallas import tpu as pltpu
from jax.sharding import PartitionSpec as P

HEAD_WIDTH = 128
MESH = pl.DeviceIdType.MESH
CAP = 50.0
IN_SCALE = 1.0 / (12.0 * CAP)
OUT_SCALE = CAP * math.log2(math.e)
HIDDEN = -4096.0


def flip(index, step, size):
    out, bit = 0, 1
    while bit < size:
        mine = (index // bit) % 2
        turn = (step // bit) % 2
        out = out + (mine + turn - 2 * mine * turn) * bit
        bit *= 2
    return out


def kernel(
    n_head, n_ctx, pair,
    order, query, key, value, out,
    qbuf, kv, acc,
    q_sent, kv_sent, x_sent, p_sent,
    q_recv, kv_recv, x_recv, p_recv, local_sem,
):
    me = lax.axis_index("head")
    ctx = lax.axis_index("ctx")
    chip, core = ctx // 2, ctx % 2
    partner = chip * 2 + 1 - core
    chips = n_ctx // 2
    pieces = n_head // pair
    rows = query.shape[0]
    total = rows * n_head
    block = total // 2
    q_cols = query.shape[1] // n_head
    kv_cols = key.shape[1] // n_head
    kv_heads = kv_cols // HEAD_WIDTH
    per_kv = q_cols // kv_cols
    h_cols = per_kv * HEAD_WIDTH
    piece_rows = rows * pair
    near_pieces = pieces // 2
    near = n_head // 2
    home = me // pair
    near_half = home // near_pieces
    far_half = 1 - near_half
    inner = (home + home // near_pieces) % 2
    same_core = [((chip + t) % chips) * 2 + core for t in range(chips)]
    other_core = [((chip + t) % chips) * 2 + 1 - core for t in range(chips)]
    peers = [flip(me, j, n_head) for j in range(1, n_head)]

    barrier = pltpu.get_barrier_semaphore()
    for d in peers:
        pl.semaphore_signal(barrier, inc=1, device_id={"head": d}, device_id_type=MESH)
    for c in [partner] + same_core[1:]:
        pl.semaphore_signal(barrier, inc=1, device_id={"ctx": c}, device_id_type=MESH)
    def rows_of(s):
        return pl.ds(pl.multiple_of(s * rows, rows), rows)

    def cols_of(s, width):
        return pl.ds(pl.multiple_of(s * width, width), width)

    mine = [
        pltpu.make_async_copy(key.at[:, cols_of(me, kv_cols)], kv.at[ctx, 0, rows_of(me)], local_sem.at[0]),
        pltpu.make_async_copy(value.at[:, cols_of(me, kv_cols)], kv.at[ctx, 1, rows_of(me)], local_sem.at[0]),
        pltpu.make_async_copy(query.at[:, cols_of(me, q_cols)], qbuf.at[rows_of(me)], local_sem.at[1]),
    ]
    for copy in mine:
        copy.start()

    pl.semaphore_wait(barrier, n_head - 1 + chips)

    def kv_sends(d):
        return [
            pltpu.make_async_remote_copy(
                src_ref=src.at[:, cols_of(d, kv_cols)], dst_ref=kv.at[ctx, i, rows_of(me)],
                send_sem=kv_sent, recv_sem=kv_recv.at[me],
                device_id={"head": d}, device_id_type=MESH,
            )
            for i, src in enumerate((key, value))
        ]

    def q_send(d, h, heads):
        return pltpu.make_async_remote_copy(
            src_ref=query.at[:, pl.ds(pl.multiple_of(d * q_cols + h * h_cols, h_cols), heads * h_cols)],
            dst_ref=qbuf.at[rows_of(me), h * h_cols : (h + heads) * h_cols],
            send_sem=q_sent, recv_sem=q_recv.at[h, me // pair],
            device_id={"head": d}, device_id_type=MESH,
        )

    sends = [copy for d in peers[near - 1 :] for copy in kv_sends(d)]
    sends += [copy for d in peers[: near - 1] for copy in kv_sends(d)]
    sends += [q_send(d, 0, kv_heads) for d in peers[: near - 1]]
    ordered = [far_half * near + i // pair * pair + flip(me % pair, i % pair, pair) for i in range(near)]
    sends += [q_send(d, h, 1) for h in range(kv_heads) for d in ordered]
    for copy in sends:
        copy.start()

    def arrived(ref, sem):
        pltpu.make_async_copy(ref, ref, sem).wait()

    def kv_ref(c, s):
        return kv.at[c, :, rows_of(s)]

    def pass_on(c, s, dest, send, recv):
        copy = pltpu.make_async_remote_copy(
            src_ref=kv_ref(c, s), dst_ref=kv_ref(c, s),
            send_sem=send, recv_sem=recv,
            device_id={"ctx": dest}, device_id_type=MESH,
        )
        copy.start()

    def to_partner(c, s):
        pass_on(c, s, partner, p_sent, p_recv.at[c // 2, s // near])

    def spread(j):
        s = flip(me, j, n_head)
        arrived(kv_ref(ctx, s), local_sem.at[0] if isinstance(j, int) and j == 0 else kv_recv.at[s])
        for c in same_core[1:]:
            pass_on(ctx, s, c, x_sent, x_recv.at[chip, s])
        to_partner(ctx, s)

    def relay(j):
        s = flip(me, j, n_head)
        for c in same_core[1:]:
            arrived(kv_ref(c, s), x_recv.at[c // 2, s])
            to_partner(c, s)

    def from_partner(half):
        for c in other_core:
            span = pl.ds(pl.multiple_of(half * block, block), block)
            arrived(kv.at[c, :, span], p_recv.at[c // 2, half])

    ones = jnp.ones((2 * block, HEAD_WIDTH), jnp.bfloat16)

    def unit(h, first_row, half, t, diagonal):
        q_half = first_row // block
        q_block = order[2 * ctx + q_half]
        c0 = ((chip + t) % chips) * 2 + core
        c1 = ((chip + t) % chips) * 2 + 1 - core
        q_span = pl.ds(pl.multiple_of(first_row, piece_rows), piece_rows)
        k_span = pl.ds(pl.multiple_of(half * block, block), block)
        low = jnp.where(order[2 * c0 + half] <= q_block, 0.0, HIDDEN)
        high = jnp.where(order[2 * c1 + half] <= q_block, 0.0, HIDDEN)
        cols = slice(h * HEAD_WIDTH, (h + 1) * HEAD_WIDTH)
        q = jnp.concatenate(
            [qbuf[q_span, (h * per_kv + i) * HEAD_WIDTH : (h * per_kv + i + 1) * HEAD_WIDTH] for i in range(per_kv)],
            axis=0,
        )
        k = jnp.concatenate([kv[c0, 0, k_span, cols], kv[c1, 0, k_span, cols]], axis=0)
        v = jnp.concatenate([kv[c0, 1, k_span, cols], kv[c1, 1, k_span, cols]], axis=0)
        x = lax.dot_general(q, k, (((1,), (1,)), ((), ())), preferred_element_type=jnp.float32)
        x = jnp.tanh(x * IN_SCALE) * OUT_SCALE
        if diagonal:
            q_at = first_row - q_half * block + lax.broadcasted_iota(jnp.int32, (piece_rows, block), 0)
            visible = lax.broadcasted_iota(jnp.int32, (piece_rows, block), 1) <= q_at
            e = jnp.exp2(x[:, :block]).reshape(per_kv, piece_rows, block)
            left = jnp.where(visible[None], e, 0.0).reshape(per_kv * piece_rows, block)
        else:
            left = jnp.exp2(x[:, :block] + low)
        w = jnp.concatenate([left, jnp.exp2(x[:, block:] + high)], axis=1).astype(jnp.bfloat16)
        return jnp.dot(w, jnp.concatenate([v, ones], axis=1), preferred_element_type=jnp.float32)

    def q_arrived(step, h, heads):
        p = flip(home, step, pieces)
        count = pair
        first = p * pair
        if isinstance(step, int) and step == 0:
            mine[2].wait()
            first, count = flip(me, 1, n_head), pair - 1
        arrived(qbuf.at[pl.ds(pl.multiple_of(first * rows, rows), count * rows), h * h_cols : (h + heads) * h_cols], q_recv.at[h, p])

    def finish(h, first_row, at):
        span = pl.ds(pl.multiple_of(first_row, piece_rows), piece_rows)
        a = acc[at, h]
        o = (a[:, :HEAD_WIDTH] / a[:, HEAD_WIDTH:]).astype(jnp.bfloat16)
        for i in range(per_kv):
            col = (h * per_kv + i) * HEAD_WIDTH
            out[span, col : col + HEAD_WIDTH] = o[i * piece_rows : (i + 1) * piece_rows]

    def each(count, body):
        lax.fori_loop(0, count, lambda i, carry: (body(i), carry)[1], 0)

    near_steps = range(near_pieces)
    far_steps = [near_pieces + flip(1 - inner, k, near_pieces) for k in near_steps]

    def far_peers(k):
        return [far_steps[k] * pair + t for t in range(pair)]

    def near_near(step):
        q_arrived(step, 0, kv_heads)
        first_row = flip(home, step, pieces) * piece_rows
        for h in range(kv_heads):
            acc[step, h] = unit(h, first_row, near_half, 0, True)

        def more(t):
            for h in range(kv_heads):
                acc[step, h] += unit(h, first_row, near_half, t + 1, False)

        each(chips - 1, more)

    for j in range(pair):
        spread(j)

    @pl.when(inner == 0)
    def _():
        for j in range(pair, near):
            spread(j)

    for j in far_peers(0):
        spread(j)

    @pl.when(inner == 1)
    def _():
        for j in range(pair, near):
            spread(j)

    for k in near_steps[1:]:
        for j in far_peers(k):
            spread(j)
    for j in range(near):
        relay(j)
    from_partner(near_half)
    near_near(0)
    for j in far_peers(0):
        relay(j)
    for step in near_steps[1:]:
        near_near(step)
    for k in near_steps[1:]:
        for j in far_peers(k):
            relay(j)
    from_partner(far_half)

    def rest(step):
        first_row = flip(home, step, pieces) * piece_rows
        def more(t):
            for h in range(kv_heads):
                acc[step, h] += unit(h, first_row, far_half, t, False)

        each(chips, more)
        for h in range(kv_heads):
            finish(h, first_row, step)

    each(near_pieces, rest)

    for h in range(kv_heads):
        def far_all(k):
            step = near_pieces + flip(1 - inner, k, near_pieces)
            q_arrived(step, h, 1)
            first_row = flip(home, step, pieces) * piece_rows
            acc[near_pieces, h] = unit(h, first_row, far_half, 0, True) + unit(h, first_row, near_half, 0, False)

            def more(t):
                acc[near_pieces, h] += unit(h, first_row, far_half, t + 1, False) + unit(h, first_row, near_half, t + 1, False)

            each(chips - 1, more)
            finish(h, first_row, near_pieces)

        each(near_pieces, far_all)
    arrived(kv.at[ctx, :, : (n_head - 1) * rows], kv_sent)
    arrived(qbuf.at[: (n_head - 1) * rows], q_sent)
    if chips > 1:
        arrived(kv.at[: chips - 1], x_sent)
    arrived(kv.at[:chips], p_sent)


def shards(n_head, n_ctx, query, key, value, block_order):
    rows = query.shape[0]
    total = rows * n_head
    q_cols = query.shape[1] // n_head
    kv_cols = key.shape[1] // n_head
    kv_heads = kv_cols // HEAD_WIDTH
    per_kv = q_cols // kv_cols
    pair = 2
    pieces = n_head // pair
    hbm = pl.BlockSpec(memory_space=pltpu.HBM)
    dma = pltpu.SemaphoreType.DMA
    return pl.pallas_call(
        functools.partial(kernel, n_head, n_ctx, pair),
        out_shape=pltpu.VMEM((total, q_cols), jnp.bfloat16),
        in_specs=[pl.BlockSpec(memory_space=pltpu.SMEM), hbm, hbm, hbm],
        out_specs=pl.BlockSpec(memory_space=pltpu.VMEM),
        scratch_shapes=[
            pltpu.VMEM((total, q_cols), jnp.bfloat16),
            pltpu.VMEM((n_ctx, 2, total, kv_cols), jnp.bfloat16),
            pltpu.VMEM((pieces // 2 + 1, kv_heads, per_kv * pair * rows, 2 * HEAD_WIDTH), jnp.float32),
            dma(()), dma(()), dma(()), dma(()),
            dma((kv_heads, pieces)), dma((n_head,)), dma((n_ctx // 2, n_head)), dma((n_ctx // 2, 2)), dma((2,)),
        ],
        compiler_params=pltpu.CompilerParams(
            collective_id=0, has_side_effects=True, vmem_limit_bytes=60 * 1024 * 1024
        ),
    )(block_order, query, key, value)


def solution(mesh):
    placed = (P(("ctx", "head"), None), P(("ctx", "head"), None), P(("ctx", "head"), None), P())
    return jax.shard_map(
        functools.partial(shards, mesh.shape["head"], mesh.shape["ctx"]),
        mesh=mesh, in_specs=placed, out_specs=P("ctx", "head"), check_vma=False,
    )
```

```python
import functools
import math

import jax
import jax.numpy as jnp
from jax import lax
from jax.experimental import pallas as pl
from jax.experimental.pallas import tpu as pltpu
from jax.sharding import PartitionSpec as P

HEAD_WIDTH = 128
MESH = pl.DeviceIdType.MESH
CAP = 50.0
IN_SCALE = 1.0 / (12.0 * CAP)
OUT_SCALE = CAP * math.log2(math.e)
HIDDEN = -4096.0


def flip(index, step, size):
    out, bit = 0, 1
    while bit < size:
        mine = (index // bit) % 2
        turn = (step // bit) % 2
        out = out + (mine + turn - 2 * mine * turn) * bit
        bit *= 2
    return out


def kernel(
    n_head, n_ctx, pair,
    order, query, key, value, out,
    qbuf, kv, acc,
    q_sent, kv_sent, x_sent, p_sent,
    q_recv, kv_recv, x_recv, p_recv, local_sem,
    head_ready, ctx_ready,
):
    me = lax.axis_index("head")
    ctx = lax.axis_index("ctx")
    chip, core = ctx // 2, ctx % 2
    partner = chip * 2 + 1 - core
    chips = n_ctx // 2
    pieces = n_head // pair
    rows = query.shape[0]
    total = rows * n_head
    block = total // 2
    q_cols = query.shape[1] // n_head
    kv_cols = key.shape[1] // n_head
    kv_heads = kv_cols // HEAD_WIDTH
    per_kv = q_cols // kv_cols
    h_cols = per_kv * HEAD_WIDTH
    piece_rows = rows * pair
    near_pieces = pieces // 2
    near = n_head // 2
    home = me // pair
    near_half = home // near_pieces
    far_half = 1 - near_half
    inner = (home + home // near_pieces) % 2
    same_core = [((chip + t) % chips) * 2 + core for t in range(chips)]
    other_core = [((chip + t) % chips) * 2 + 1 - core for t in range(chips)]
    peers = [flip(me, j, n_head) for j in range(1, n_head)]

    others = [("head", d) for d in peers] + [("ctx", c) for c in [partner] + same_core[1:]]
    at = {"head": me, "ctx": ctx}
    ready = {"head": head_ready, "ctx": ctx_ready}

    def tell(sem, axis, d):
        pl.semaphore_signal(sem, inc=1, device_id={axis: d}, device_id_type=MESH)

    def met(axis, d):
        @pl.when(d > at[axis])
        def _():
            pl.semaphore_wait(ready[axis].at[d], 1)

    barrier = pltpu.get_barrier_semaphore()
    for axis, d in others:
        @pl.when(d > at[axis])
        def _():
            tell(barrier, axis, d)

    def rows_of(s):
        return pl.ds(pl.multiple_of(s * rows, rows), rows)

    def cols_of(s, width):
        return pl.ds(pl.multiple_of(s * width, width), width)

    mine = [
        pltpu.make_async_copy(key.at[:, cols_of(me, kv_cols)], kv.at[ctx, 0, rows_of(me)], local_sem.at[0]),
        pltpu.make_async_copy(value.at[:, cols_of(me, kv_cols)], kv.at[ctx, 1, rows_of(me)], local_sem.at[0]),
        pltpu.make_async_copy(query.at[:, cols_of(me, q_cols)], qbuf.at[rows_of(me)], local_sem.at[1]),
    ]
    for copy in mine:
        copy.start()

    @pl.when(me + chip + core > 0)
    def _():
        pl.semaphore_wait(barrier, me + chip + core)

    for axis, d in others:
        @pl.when(d < at[axis])
        def _():
            tell(ready[axis].at[at[axis]], axis, d)


    def kv_sends(d):
        return [
            pltpu.make_async_remote_copy(
                src_ref=src.at[:, cols_of(d, kv_cols)], dst_ref=kv.at[ctx, i, rows_of(me)],
                send_sem=kv_sent, recv_sem=kv_recv.at[me],
                device_id={"head": d}, device_id_type=MESH,
            )
            for i, src in enumerate((key, value))
        ]

    def q_send(d, h, heads):
        return pltpu.make_async_remote_copy(
            src_ref=query.at[:, pl.ds(pl.multiple_of(d * q_cols + h * h_cols, h_cols), heads * h_cols)],
            dst_ref=qbuf.at[rows_of(me), h * h_cols : (h + heads) * h_cols],
            send_sem=q_sent, recv_sem=q_recv.at[h, me // pair],
            device_id={"head": d}, device_id_type=MESH,
        )

    def arrived(ref, sem):
        pltpu.make_async_copy(ref, ref, sem).wait()

    def kv_ref(c, s):
        return kv.at[c, :, rows_of(s)]

    def pass_on(c, s, dest, send, recv):
        copy = pltpu.make_async_remote_copy(
            src_ref=kv_ref(c, s), dst_ref=kv_ref(c, s),
            send_sem=send, recv_sem=recv,
            device_id={"ctx": dest}, device_id_type=MESH,
        )
        copy.start()

    def to_partner(c, s):
        pass_on(c, s, partner, p_sent, p_recv.at[c // 2, s // near])

    def spread(j):
        s = flip(me, j, n_head)
        arrived(kv_ref(ctx, s), local_sem.at[0] if isinstance(j, int) and j == 0 else kv_recv.at[s])
        for c in same_core[1:]:
            pass_on(ctx, s, c, x_sent, x_recv.at[chip, s])
        to_partner(ctx, s)

    def relay(j):
        s = flip(me, j, n_head)
        for c in same_core[1:]:
            arrived(kv_ref(c, s), x_recv.at[c // 2, s])
            to_partner(c, s)

    def from_partner(half):
        for c in other_core:
            span = pl.ds(pl.multiple_of(half * block, block), block)
            arrived(kv.at[c, :, span], p_recv.at[c // 2, half])

    near_js, far_js = list(range(1, near)), list(range(near, n_head))

    def send_kv(js):
        for j in js:
            met("head", peers[j - 1])
            for copy in kv_sends(peers[j - 1]):
                copy.start()

    @pl.when(near_half == 1)
    def _():
        send_kv(far_js)

    for c in [partner] + same_core[1:]:
        met("ctx", c)
    spread(0)

    @pl.when(near_half == 1)
    def _():
        send_kv(near_js)

    @pl.when((near_half == 0) & (inner == 0))
    def _():
        send_kv(near_js[: pair - 1] + far_js[: near // 2] + near_js[pair - 1 :] + far_js[near // 2 :])

    @pl.when((near_half == 0) & (inner == 1))
    def _():
        send_kv(far_js[near // 2 :] + near_js + far_js[: near // 2])

    ordered = [far_half * near + i // pair * pair + flip(me % pair, i % pair, pair) for i in range(near)]
    sends = [q_send(d, 0, kv_heads) for d in peers[: near - 1]]
    sends += [q_send(d, h, 1) for h in range(kv_heads) for d in ordered]
    for copy in sends:
        copy.start()

    ones = jnp.ones((2 * block, HEAD_WIDTH), jnp.bfloat16)

    def unit(h, first_row, m, half, t, diagonal):
        q_half = first_row // block
        q_block = order[2 * ctx + q_half]
        c0 = ((chip + t) % chips) * 2 + core
        c1 = ((chip + t) % chips) * 2 + 1 - core
        q_span = pl.ds(pl.multiple_of(first_row, piece_rows), m)
        k_span = pl.ds(pl.multiple_of(half * block, block), block)
        low = jnp.where(order[2 * c0 + half] <= q_block, 0.0, HIDDEN)
        high = jnp.where(order[2 * c1 + half] <= q_block, 0.0, HIDDEN)
        cols = slice(h * HEAD_WIDTH, (h + 1) * HEAD_WIDTH)
        q = jnp.concatenate(
            [qbuf[q_span, (h * per_kv + i) * HEAD_WIDTH : (h * per_kv + i + 1) * HEAD_WIDTH] for i in range(per_kv)],
            axis=0,
        )
        k = jnp.concatenate([kv[c0, 0, k_span, cols], kv[c1, 0, k_span, cols]], axis=0)
        v = jnp.concatenate([kv[c0, 1, k_span, cols], kv[c1, 1, k_span, cols]], axis=0)
        x = lax.dot_general(q, k, (((1,), (1,)), ((), ())), preferred_element_type=jnp.float32)
        x = jnp.tanh(x * IN_SCALE) * OUT_SCALE
        if diagonal:
            q_at = first_row - q_half * block + lax.broadcasted_iota(jnp.int32, (m, block), 0)
            visible = lax.broadcasted_iota(jnp.int32, (m, block), 1) <= q_at
            e = jnp.exp2(x[:, :block]).reshape(per_kv, m, block)
            left = jnp.where(visible[None], e, 0.0).reshape(per_kv * m, block)
        else:
            left = jnp.exp2(x[:, :block] + low)
        w = jnp.concatenate([left, jnp.exp2(x[:, block:] + high)], axis=1).astype(jnp.bfloat16)
        return jnp.dot(w, jnp.concatenate([v, ones], axis=1), preferred_element_type=jnp.float32)

    def q_arrived(step, h, heads):
        p = flip(home, step, pieces)
        count = pair
        first = p * pair
        if isinstance(step, int) and step == 0:
            mine[2].wait()
            first, count = flip(me, 1, n_head), pair - 1
        arrived(qbuf.at[pl.ds(pl.multiple_of(first * rows, rows), count * rows), h * h_cols : (h + heads) * h_cols], q_recv.at[h, p])

    def finish(h, first_row, m, a):
        span = pl.ds(pl.multiple_of(first_row, piece_rows), m)
        o = (a[:, :HEAD_WIDTH] / a[:, HEAD_WIDTH:]).astype(jnp.bfloat16)
        for i in range(per_kv):
            col = (h * per_kv + i) * HEAD_WIDTH
            out[span, col : col + HEAD_WIDTH] = o[i * m : (i + 1) * m]

    def each(count, body):
        lax.fori_loop(0, count, lambda i, carry: (body(i), carry)[1], 0)

    near_steps = range(near_pieces)
    far_steps = [near_pieces + flip(1 - inner, k, near_pieces) for k in near_steps]

    def far_peers(k):
        return [far_steps[k] * pair + t for t in range(pair)]

    near_row, far_row = near_half * block, far_half * block

    def add_up(h, first_row, m, halves, diagonal, start):
        a = acc.at[h, : per_kv * m]
        o = sum(unit(h, first_row, m, half, 0, diagonal and half is halves[0]) for half in halves)
        a[...] = o if start else a[...] + o

        def more(t):
            a[...] += sum(unit(h, first_row, m, half, t + 1, False) for half in halves)

        each(chips - 1, more)

    def pass_far(k):
        for j in far_peers(k):
            relay(j)

    for j in range(1, pair):
        spread(j)

    @pl.when(inner == 0)
    def _():
        for j in range(pair, near):
            spread(j)

    for j in far_peers(0):
        spread(j)

    @pl.when(inner == 1)
    def _():
        for j in range(pair, near):
            spread(j)

    for k in near_steps[1:]:
        for j in far_peers(k):
            spread(j)
    for j in range(near):
        relay(j)

    @pl.when(core == 1)
    def _():
        for k in near_steps[:-1]:
            pass_far(k)

    from_partner(near_half)
    for step in near_steps:
        q_arrived(step, 0, kv_heads)
    for h in range(kv_heads):
        add_up(h, near_row, block, [near_half], True, True)
        if h == 0:
            @pl.when(core == 0)
            def _():
                for k in near_steps[:-1]:
                    pass_far(k)

            pass_far(near_pieces - 1)
    from_partner(far_half)
    for h in range(kv_heads):
        add_up(h, near_row, block, [far_half], False, False)
        finish(h, near_row, block, acc[h])
    for h in range(kv_heads):
        def far(k):
            step = near_pieces + flip(1 - inner, k, near_pieces)
            q_arrived(step, h, 1)
            first_row = flip(home, step, pieces) * piece_rows
            add_up(h, first_row, piece_rows, [far_half, near_half], True, True)
            finish(h, first_row, piece_rows, acc[h, : per_kv * piece_rows])

        each(near_pieces, far)
    arrived(kv.at[ctx, :, : (n_head - 1) * rows], kv_sent)
    arrived(qbuf.at[: (n_head - 1) * rows], q_sent)
    if chips > 1:
        arrived(kv.at[: chips - 1], x_sent)
    arrived(kv.at[:chips], p_sent)


def shards(n_head, n_ctx, query, key, value, block_order):
    rows = query.shape[0]
    total = rows * n_head
    q_cols = query.shape[1] // n_head
    kv_cols = key.shape[1] // n_head
    kv_heads = kv_cols // HEAD_WIDTH
    per_kv = q_cols // kv_cols
    pair = 2
    pieces = n_head // pair
    hbm = pl.BlockSpec(memory_space=pltpu.HBM)
    dma = pltpu.SemaphoreType.DMA
    return pl.pallas_call(
        functools.partial(kernel, n_head, n_ctx, pair),
        out_shape=pltpu.VMEM((total, q_cols), jnp.bfloat16),
        in_specs=[pl.BlockSpec(memory_space=pltpu.SMEM), hbm, hbm, hbm],
        out_specs=pl.BlockSpec(memory_space=pltpu.VMEM),
        scratch_shapes=[
            pltpu.VMEM((total, q_cols), jnp.bfloat16),
            pltpu.VMEM((n_ctx, 2, total, kv_cols), jnp.bfloat16),
            pltpu.VMEM((kv_heads, per_kv * total // 2, 2 * HEAD_WIDTH), jnp.float32),
            dma(()), dma(()), dma(()), dma(()),
            dma((kv_heads, pieces)), dma((n_head,)), dma((n_ctx // 2, n_head)), dma((n_ctx // 2, 2)), dma((2,)),
            pltpu.SemaphoreType.REGULAR((n_head,)), pltpu.SemaphoreType.REGULAR((n_ctx,)),
        ],
        compiler_params=pltpu.CompilerParams(
            collective_id=0, has_side_effects=True, vmem_limit_bytes=60 * 1024 * 1024
        ),
    )(block_order, query, key, value)


def solution(mesh):
    placed = (P(("ctx", "head"), None), P(("ctx", "head"), None), P(("ctx", "head"), None), P())
    return jax.shard_map(
        functools.partial(shards, mesh.shape["head"], mesh.shape["ctx"]),
        mesh=mesh, in_specs=placed, out_specs=P("ctx", "head"), check_vma=False,
    )
```

```python
import functools
import math

import jax
import jax.numpy as jnp
from jax import lax
from jax.experimental import pallas as pl
from jax.experimental.pallas import tpu as pltpu
from jax.sharding import PartitionSpec as P

HEAD_WIDTH = 128
MESH = pl.DeviceIdType.MESH
CAP = 50.0
IN_SCALE = 1.0 / (12.0 * CAP)
OUT_SCALE = CAP * math.log2(math.e)
HIDDEN = -4096.0


def flip(index, step, size):
    out, bit = 0, 1
    while bit < size:
        mine = (index // bit) % 2
        turn = (step // bit) % 2
        out = out + (mine + turn - 2 * mine * turn) * bit
        bit *= 2
    return out


def kernel(
    n_head, n_ctx, pair,
    order, query, key, value, out,
    qbuf, kv, acc,
    q_sent, kv_sent, x_sent, p_sent,
    q_recv, kv_recv, x_recv, p_recv, local_sem,
    head_ready, ctx_ready,
):
    me = lax.axis_index("head")
    ctx = lax.axis_index("ctx")
    chip, core = ctx // 2, ctx % 2
    partner = chip * 2 + 1 - core
    chips = n_ctx // 2
    pieces = n_head // pair
    rows = query.shape[0]
    total = rows * n_head
    block = total // 2
    q_cols = query.shape[1] // n_head
    kv_cols = key.shape[1] // n_head
    kv_heads = kv_cols // HEAD_WIDTH
    per_kv = q_cols // kv_cols
    h_cols = per_kv * HEAD_WIDTH
    piece_rows = rows * pair
    near_pieces = pieces // 2
    near = n_head // 2
    home = me // pair
    near_half = home // near_pieces
    far_half = 1 - near_half
    inner = (home + home // near_pieces) % 2
    same_core = [((chip + t) % chips) * 2 + core for t in range(chips)]
    other_core = [((chip + t) % chips) * 2 + 1 - core for t in range(chips)]
    peers = [flip(me, j, n_head) for j in range(1, n_head)]

    others = [("head", d) for d in peers] + [("ctx", c) for c in [partner] + same_core[1:]]
    at = {"head": me, "ctx": ctx}
    ready = {"head": head_ready, "ctx": ctx_ready}

    def tell(sem, axis, d):
        pl.semaphore_signal(sem, inc=1, device_id={axis: d}, device_id_type=MESH)

    def met(axis, d):
        @pl.when(d > at[axis])
        def _():
            pl.semaphore_wait(ready[axis].at[d], 1)

    barrier = pltpu.get_barrier_semaphore()
    for axis, d in others:
        @pl.when(d > at[axis])
        def _():
            tell(barrier, axis, d)

    def rows_of(s):
        return pl.ds(pl.multiple_of(s * rows, rows), rows)

    def cols_of(s, width):
        return pl.ds(pl.multiple_of(s * width, width), width)

    mine = [
        pltpu.make_async_copy(key.at[:, cols_of(me, kv_cols)], kv.at[ctx, 0, rows_of(me)], local_sem.at[0]),
        pltpu.make_async_copy(value.at[:, cols_of(me, kv_cols)], kv.at[ctx, 1, rows_of(me)], local_sem.at[0]),
        pltpu.make_async_copy(query.at[:, cols_of(me, q_cols)], qbuf.at[rows_of(me)], local_sem.at[1]),
    ]
    for copy in mine:
        copy.start()

    @pl.when(me + chip + core > 0)
    def _():
        pl.semaphore_wait(barrier, me + chip + core)

    for axis, d in others:
        @pl.when(d < at[axis])
        def _():
            tell(ready[axis].at[at[axis]], axis, d)


    def kv_sends(d):
        return [
            pltpu.make_async_remote_copy(
                src_ref=src.at[:, cols_of(d, kv_cols)], dst_ref=kv.at[ctx, i, rows_of(me)],
                send_sem=kv_sent, recv_sem=kv_recv.at[me],
                device_id={"head": d}, device_id_type=MESH,
            )
            for i, src in enumerate((key, value))
        ]

    def q_send(d, h, heads):
        return pltpu.make_async_remote_copy(
            src_ref=query.at[:, pl.ds(pl.multiple_of(d * q_cols + h * h_cols, h_cols), heads * h_cols)],
            dst_ref=qbuf.at[rows_of(me), h * h_cols : (h + heads) * h_cols],
            send_sem=q_sent, recv_sem=q_recv.at[h, me // pair],
            device_id={"head": d}, device_id_type=MESH,
        )

    def arrived(ref, sem):
        pltpu.make_async_copy(ref, ref, sem).wait()

    def kv_ref(c, s):
        return kv.at[c, :, rows_of(s)]

    def pass_on(c, s, dest, send, recv):
        copy = pltpu.make_async_remote_copy(
            src_ref=kv_ref(c, s), dst_ref=kv_ref(c, s),
            send_sem=send, recv_sem=recv,
            device_id={"ctx": dest}, device_id_type=MESH,
        )
        copy.start()

    def to_partner(c, s):
        pass_on(c, s, partner, p_sent, p_recv.at[c // 2, s // near])

    def spread(j):
        s = flip(me, j, n_head)
        arrived(kv_ref(ctx, s), local_sem.at[0] if isinstance(j, int) and j == 0 else kv_recv.at[s])
        for c in same_core[1:]:
            pass_on(ctx, s, c, x_sent, x_recv.at[chip, s])
        to_partner(ctx, s)

    def relay(j):
        s = flip(me, j, n_head)
        for c in same_core[1:]:
            arrived(kv_ref(c, s), x_recv.at[c // 2, s])
            to_partner(c, s)

    def from_partner(half):
        for c in other_core:
            span = pl.ds(pl.multiple_of(half * block, block), block)
            arrived(kv.at[c, :, span], p_recv.at[c // 2, half])

    near_js, far_js = list(range(1, near)), list(range(near, n_head))

    def send_kv(js):
        for j in js:
            met("head", peers[j - 1])
            for copy in kv_sends(peers[j - 1]):
                copy.start()

    @pl.when(near_half == 1)
    def _():
        send_kv(far_js)

    for c in [partner] + same_core[1:]:
        met("ctx", c)
    spread(0)

    @pl.when(near_half == 1)
    def _():
        send_kv(near_js)

    @pl.when((near_half == 0) & (inner == 0))
    def _():
        send_kv(near_js[: pair - 1] + far_js[: near // 2] + near_js[pair - 1 :] + far_js[near // 2 :])

    @pl.when((near_half == 0) & (inner == 1))
    def _():
        send_kv(far_js[near // 2 :] + near_js + far_js[: near // 2])

    ordered = [far_half * near + i for i in range(near)]
    sends = [q_send(d, 0, kv_heads) for d in peers[: near - 1]]
    sends += [q_send(d, h, 1) for h in range(kv_heads) for d in ordered]
    for copy in sends:
        copy.start()

    ones = jnp.ones((2 * block, HEAD_WIDTH), jnp.bfloat16)

    def unit(h, first_row, m, half, t, diagonal):
        q_half = first_row // block
        q_block = order[2 * ctx + q_half]
        c0 = ((chip + t) % chips) * 2 + core
        c1 = ((chip + t) % chips) * 2 + 1 - core
        q_span = pl.ds(pl.multiple_of(first_row, piece_rows), m)
        k_span = pl.ds(pl.multiple_of(half * block, block), block)
        low = jnp.where(order[2 * c0 + half] <= q_block, 0.0, HIDDEN)
        high = jnp.where(order[2 * c1 + half] <= q_block, 0.0, HIDDEN)
        cols = slice(h * HEAD_WIDTH, (h + 1) * HEAD_WIDTH)
        q = jnp.concatenate(
            [qbuf[q_span, (h * per_kv + i) * HEAD_WIDTH : (h * per_kv + i + 1) * HEAD_WIDTH] for i in range(per_kv)],
            axis=0,
        )
        k = jnp.concatenate([kv[c0, 0, k_span, cols], kv[c1, 0, k_span, cols]], axis=0)
        v = jnp.concatenate([kv[c0, 1, k_span, cols], kv[c1, 1, k_span, cols]], axis=0)
        x = lax.dot_general(q, k, (((1,), (1,)), ((), ())), preferred_element_type=jnp.float32)
        x = jnp.tanh(x * IN_SCALE) * OUT_SCALE
        if diagonal:
            q_at = first_row - q_half * block + lax.broadcasted_iota(jnp.int32, (m, block), 0)
            visible = lax.broadcasted_iota(jnp.int32, (m, block), 1) <= q_at
            e = jnp.exp2(x[:, :block]).reshape(per_kv, m, block)
            left = jnp.where(visible[None], e, 0.0).reshape(per_kv * m, block)
        else:
            left = jnp.exp2(x[:, :block] + low)
        w = jnp.concatenate([left, jnp.exp2(x[:, block:] + high)], axis=1).astype(jnp.bfloat16)
        return jnp.dot(w, jnp.concatenate([v, ones], axis=1), preferred_element_type=jnp.float32)

    def q_arrived(step, h, heads):
        p = flip(home, step, pieces)
        count = pair
        first = p * pair
        if isinstance(step, int) and step == 0:
            mine[2].wait()
            first, count = flip(me, 1, n_head), pair - 1
        arrived(qbuf.at[pl.ds(pl.multiple_of(first * rows, rows), count * rows), h * h_cols : (h + heads) * h_cols], q_recv.at[h, p])

    def finish(h, first_row, m, a):
        span = pl.ds(pl.multiple_of(first_row, piece_rows), m)
        o = (a[:, :HEAD_WIDTH] / a[:, HEAD_WIDTH:]).astype(jnp.bfloat16)
        for i in range(per_kv):
            col = (h * per_kv + i) * HEAD_WIDTH
            out[span, col : col + HEAD_WIDTH] = o[i * m : (i + 1) * m]

    def each(count, body):
        lax.fori_loop(0, count, lambda i, carry: (body(i), carry)[1], 0)

    near_steps = range(near_pieces)
    far_steps = [near_pieces + flip(1 - inner, k, near_pieces) for k in near_steps]

    def far_peers(k):
        return [far_steps[k] * pair + t for t in range(pair)]

    near_row, far_row = near_half * block, far_half * block

    def add_up(h, first_row, m, halves, diagonal, start):
        a = acc.at[h, : per_kv * m]
        o = sum(unit(h, first_row, m, half, 0, diagonal and half is halves[0]) for half in halves)
        a[...] = o if start else a[...] + o

        def more(t):
            a[...] += sum(unit(h, first_row, m, half, t + 1, False) for half in halves)

        each(chips - 1, more)

    def pass_far(k):
        for j in far_peers(k):
            relay(j)

    later = (inner == 1) | ((near_half == 0) & (core == 0))

    for j in range(1, pair):
        spread(j)

    @pl.when(jnp.logical_not(later))
    def _():
        for j in range(pair, near):
            spread(j)

    for j in far_peers(0):
        spread(j)

    @pl.when(later)
    def _():
        for j in range(pair, near):
            spread(j)

    for k in near_steps[1:]:
        for j in far_peers(k):
            spread(j)
    for j in range(near):
        relay(j)

    @pl.when(core == 1)
    def _():
        for k in near_steps[:-1]:
            pass_far(k)

    from_partner(near_half)
    for step in near_steps:
        q_arrived(step, 0, kv_heads)
    for h in range(kv_heads):
        add_up(h, near_row, block, [near_half], True, True)
        if h == 0:
            @pl.when(core == 0)
            def _():
                for k in near_steps[:-1]:
                    pass_far(k)

            pass_far(near_pieces - 1)
    from_partner(far_half)
    for h in range(kv_heads):
        add_up(h, near_row, block, [far_half], False, False)
        finish(h, near_row, block, acc[h])
    for h in range(kv_heads):
        def far(k):
            step = near_pieces + flip(1 - inner, k, near_pieces)
            q_arrived(step, h, 1)
            first_row = flip(home, step, pieces) * piece_rows
            add_up(h, first_row, piece_rows, [far_half, near_half], True, True)
            finish(h, first_row, piece_rows, acc[h, : per_kv * piece_rows])

        each(near_pieces, far)
    arrived(kv.at[ctx, :, : (n_head - 1) * rows], kv_sent)
    arrived(qbuf.at[: (n_head - 1) * rows], q_sent)
    if chips > 1:
        arrived(kv.at[: chips - 1], x_sent)
    arrived(kv.at[:chips], p_sent)


def shards(n_head, n_ctx, query, key, value, block_order):
    rows = query.shape[0]
    total = rows * n_head
    q_cols = query.shape[1] // n_head
    kv_cols = key.shape[1] // n_head
    kv_heads = kv_cols // HEAD_WIDTH
    per_kv = q_cols // kv_cols
    pair = 2
    pieces = n_head // pair
    hbm = pl.BlockSpec(memory_space=pltpu.HBM)
    dma = pltpu.SemaphoreType.DMA
    return pl.pallas_call(
        functools.partial(kernel, n_head, n_ctx, pair),
        out_shape=pltpu.VMEM((total, q_cols), jnp.bfloat16),
        in_specs=[pl.BlockSpec(memory_space=pltpu.SMEM), hbm, hbm, hbm],
        out_specs=pl.BlockSpec(memory_space=pltpu.VMEM),
        scratch_shapes=[
            pltpu.VMEM((total, q_cols), jnp.bfloat16),
            pltpu.VMEM((n_ctx, 2, total, kv_cols), jnp.bfloat16),
            pltpu.VMEM((kv_heads, per_kv * total // 2, 2 * HEAD_WIDTH), jnp.float32),
            dma(()), dma(()), dma(()), dma(()),
            dma((kv_heads, pieces)), dma((n_head,)), dma((n_ctx // 2, n_head)), dma((n_ctx // 2, 2)), dma((2,)),
            pltpu.SemaphoreType.REGULAR((n_head,)), pltpu.SemaphoreType.REGULAR((n_ctx,)),
        ],
        compiler_params=pltpu.CompilerParams(
            collective_id=0, has_side_effects=True, vmem_limit_bytes=60 * 1024 * 1024
        ),
    )(block_order, query, key, value)


def solution(mesh):
    placed = (P(("ctx", "head"), None), P(("ctx", "head"), None), P(("ctx", "head"), None), P())
    return jax.shard_map(
        functools.partial(shards, mesh.shape["head"], mesh.shape["ctx"]),
        mesh=mesh, in_specs=placed, out_specs=P("ctx", "head"), check_vma=False,
    )
```

```python
import functools
import math

import jax
import jax.numpy as jnp
from jax import lax
from jax.experimental import pallas as pl
from jax.experimental.pallas import tpu as pltpu
from jax.sharding import PartitionSpec as P

HEAD_WIDTH = 128
MESH = pl.DeviceIdType.MESH
CAP = 50.0
IN_SCALE = 1.0 / (12.0 * CAP)
OUT_SCALE = CAP * math.log2(math.e)
HIDDEN = -4096.0


def flip(index, step, size):
    out, bit = 0, 1
    while bit < size:
        mine = (index // bit) % 2
        turn = (step // bit) % 2
        out = out + (mine + turn - 2 * mine * turn) * bit
        bit *= 2
    return out


def kernel(
    n_head, n_ctx, pair,
    block_order, query, key, value, out,
    qbuf, kv, acc, order,
    q_sent, kv_sent, x_sent, p_sent,
    q_recv, kv_recv, x_recv, p_recv, local_sem,
    head_ready, ctx_ready,
):
    me = lax.axis_index("head")
    ctx = lax.axis_index("ctx")
    chip, core = ctx // 2, ctx % 2
    partner = chip * 2 + 1 - core
    chips = n_ctx // 2
    pieces = n_head // pair
    rows = query.shape[0]
    total = rows * n_head
    block = total // 2
    q_cols = query.shape[1] // n_head
    kv_cols = key.shape[1] // n_head
    kv_heads = kv_cols // HEAD_WIDTH
    per_kv = q_cols // kv_cols
    h_cols = per_kv * HEAD_WIDTH
    piece_rows = rows * pair
    near_pieces = pieces // 2
    near = n_head // 2
    home = me // pair
    near_half = home // near_pieces
    far_half = 1 - near_half
    inner = (home + home // near_pieces) % 2
    same_core = [((chip + t) % chips) * 2 + core for t in range(chips)]
    other_core = [((chip + t) % chips) * 2 + 1 - core for t in range(chips)]
    peers = [flip(me, j, n_head) for j in range(1, n_head)]

    others = [("head", d) for d in peers] + [("ctx", c) for c in [partner] + same_core[1:]]
    at = {"head": me, "ctx": ctx}
    ready = {"head": head_ready, "ctx": ctx_ready}

    def tell(sem, axis, d):
        pl.semaphore_signal(sem, inc=1, device_id={axis: d}, device_id_type=MESH)

    def met(axis, d):
        @pl.when(d > at[axis])
        def _():
            pl.semaphore_wait(ready[axis].at[d], 1)

    barrier = pltpu.get_barrier_semaphore()
    for axis, d in others:
        @pl.when(d > at[axis])
        def _():
            tell(barrier, axis, d)

    def rows_of(s):
        return pl.ds(pl.multiple_of(s * rows, rows), rows)

    def cols_of(s, width):
        return pl.ds(pl.multiple_of(s * width, width), width)

    mine = [
        pltpu.make_async_copy(key.at[:, cols_of(me, kv_cols)], kv.at[ctx, 0, rows_of(me)], local_sem.at[0]),
        pltpu.make_async_copy(value.at[:, cols_of(me, kv_cols)], kv.at[ctx, 1, rows_of(me)], local_sem.at[0]),
        pltpu.make_async_copy(query.at[:, cols_of(me, q_cols)], qbuf.at[rows_of(me)], local_sem.at[1]),
    ]
    mine.append(pltpu.make_async_copy(block_order, order, local_sem.at[2]))
    for copy in mine:
        copy.start()

    @pl.when(me + chip + core > 0)
    def _():
        pl.semaphore_wait(barrier, me + chip + core)

    for axis, d in others:
        @pl.when(d < at[axis])
        def _():
            tell(ready[axis].at[at[axis]], axis, d)


    def kv_sends(d):
        return [
            pltpu.make_async_remote_copy(
                src_ref=src.at[:, cols_of(d, kv_cols)], dst_ref=kv.at[ctx, i, rows_of(me)],
                send_sem=kv_sent, recv_sem=kv_recv.at[me],
                device_id={"head": d}, device_id_type=MESH,
            )
            for i, src in enumerate((key, value))
        ]

    def q_send(d, h, heads):
        return pltpu.make_async_remote_copy(
            src_ref=query.at[:, pl.ds(pl.multiple_of(d * q_cols + h * h_cols, h_cols), heads * h_cols)],
            dst_ref=qbuf.at[rows_of(me), h * h_cols : (h + heads) * h_cols],
            send_sem=q_sent, recv_sem=q_recv.at[h, me // pair],
            device_id={"head": d}, device_id_type=MESH,
        )

    def arrived(ref, sem):
        pltpu.make_async_copy(ref, ref, sem).wait()

    def kv_ref(c, s):
        return kv.at[c, :, rows_of(s)]

    def pass_on(c, s, dest, send, recv):
        copy = pltpu.make_async_remote_copy(
            src_ref=kv_ref(c, s), dst_ref=kv_ref(c, s),
            send_sem=send, recv_sem=recv,
            device_id={"ctx": dest}, device_id_type=MESH,
        )
        copy.start()

    def to_partner(c, s):
        pass_on(c, s, partner, p_sent, p_recv.at[c // 2, s // near])

    def spread(j):
        s = flip(me, j, n_head)
        arrived(kv_ref(ctx, s), local_sem.at[0] if isinstance(j, int) and j == 0 else kv_recv.at[s])
        for c in same_core[1:]:
            pass_on(ctx, s, c, x_sent, x_recv.at[chip, s])
        to_partner(ctx, s)

    def relay(j):
        s = flip(me, j, n_head)
        for c in same_core[1:]:
            arrived(kv_ref(c, s), x_recv.at[c // 2, s])
            to_partner(c, s)

    def from_partner(half):
        for c in other_core:
            span = pl.ds(pl.multiple_of(half * block, block), block)
            arrived(kv.at[c, :, span], p_recv.at[c // 2, half])

    near_js, far_js = list(range(1, near)), list(range(near, n_head))

    def send_kv(js):
        for j in js:
            met("head", peers[j - 1])
            for copy in kv_sends(peers[j - 1]):
                copy.start()

    @pl.when(near_half == 1)
    def _():
        send_kv(far_js)

    for c in [partner] + same_core[1:]:
        met("ctx", c)
    spread(0)

    @pl.when(near_half == 1)
    def _():
        send_kv(near_js)

    @pl.when((near_half == 0) & (inner == 0))
    def _():
        send_kv(near_js[: pair - 1] + far_js[: near // 2] + near_js[pair - 1 :] + far_js[near // 2 :])

    @pl.when((near_half == 0) & (inner == 1))
    def _():
        send_kv(far_js[near // 2 :] + near_js + far_js[: near // 2])

    ordered = [far_half * near + i for i in range(near)]
    sends = [q_send(d, 0, kv_heads) for d in peers[: near - 1]]
    sends += [q_send(d, h, 1) for h in range(kv_heads) for d in ordered]
    for copy in sends:
        copy.start()

    ones = jnp.ones((2 * block, HEAD_WIDTH), jnp.bfloat16)

    def unit(h, first_row, m, half, t, diagonal):
        q_half = first_row // block
        q_block = order[2 * ctx + q_half]
        c0 = ((chip + t) % chips) * 2 + core
        c1 = ((chip + t) % chips) * 2 + 1 - core
        q_span = pl.ds(pl.multiple_of(first_row, piece_rows), m)
        k_span = pl.ds(pl.multiple_of(half * block, block), block)
        low = jnp.where(order[2 * c0 + half] <= q_block, 0.0, HIDDEN)
        high = jnp.where(order[2 * c1 + half] <= q_block, 0.0, HIDDEN)
        cols = slice(h * HEAD_WIDTH, (h + 1) * HEAD_WIDTH)
        q = jnp.concatenate(
            [qbuf[q_span, (h * per_kv + i) * HEAD_WIDTH : (h * per_kv + i + 1) * HEAD_WIDTH] for i in range(per_kv)],
            axis=0,
        )
        k = jnp.concatenate([kv[c0, 0, k_span, cols], kv[c1, 0, k_span, cols]], axis=0)
        v = jnp.concatenate([kv[c0, 1, k_span, cols], kv[c1, 1, k_span, cols]], axis=0)
        x = lax.dot_general(q, k, (((1,), (1,)), ((), ())), preferred_element_type=jnp.float32)
        x = jnp.tanh(x * IN_SCALE) * OUT_SCALE
        if diagonal:
            q_at = first_row - q_half * block + lax.broadcasted_iota(jnp.int32, (m, block), 0)
            visible = lax.broadcasted_iota(jnp.int32, (m, block), 1) <= q_at
            e = jnp.exp2(x[:, :block]).reshape(per_kv, m, block)
            left = jnp.where(visible[None], e, 0.0).reshape(per_kv * m, block)
        else:
            left = jnp.exp2(x[:, :block] + low)
        w = jnp.concatenate([left, jnp.exp2(x[:, block:] + high)], axis=1).astype(jnp.bfloat16)
        return jnp.dot(w, jnp.concatenate([v, ones], axis=1), preferred_element_type=jnp.float32)

    def q_arrived(step, h, heads):
        p = flip(home, step, pieces)
        count = pair
        first = p * pair
        if isinstance(step, int) and step == 0:
            mine[2].wait()
            first, count = flip(me, 1, n_head), pair - 1
        arrived(qbuf.at[pl.ds(pl.multiple_of(first * rows, rows), count * rows), h * h_cols : (h + heads) * h_cols], q_recv.at[h, p])

    def finish(h, first_row, m, a):
        span = pl.ds(pl.multiple_of(first_row, piece_rows), m)
        o = (a[:, :HEAD_WIDTH] / a[:, HEAD_WIDTH:]).astype(jnp.bfloat16)
        for i in range(per_kv):
            col = (h * per_kv + i) * HEAD_WIDTH
            out[span, col : col + HEAD_WIDTH] = o[i * m : (i + 1) * m]

    def each(count, body):
        lax.fori_loop(0, count, lambda i, carry: (body(i), carry)[1], 0)

    near_steps = range(near_pieces)
    far_steps = [near_pieces + flip(1 - inner, k, near_pieces) for k in near_steps]

    def far_peers(k):
        return [far_steps[k] * pair + t for t in range(pair)]

    near_row, far_row = near_half * block, far_half * block

    def add_up(h, first_row, m, halves, diagonal, start):
        a = acc.at[h, : per_kv * m]
        o = sum(unit(h, first_row, m, half, 0, diagonal and half is halves[0]) for half in halves)
        a[...] = o if start else a[...] + o

        def more(t):
            a[...] += sum(unit(h, first_row, m, half, t + 1, False) for half in halves)

        each(chips - 1, more)

    def pass_far(k):
        for j in far_peers(k):
            relay(j)

    later = (inner == 1) | ((near_half == 0) & (core == 0))

    for j in range(1, pair):
        spread(j)

    @pl.when(jnp.logical_not(later))
    def _():
        for j in range(pair, near):
            spread(j)

    for j in far_peers(0):
        spread(j)

    @pl.when(later)
    def _():
        for j in range(pair, near):
            spread(j)

    for k in near_steps[1:]:
        for j in far_peers(k):
            spread(j)
    for j in range(near):
        relay(j)

    @pl.when(core == 1)
    def _():
        for k in near_steps[:-1]:
            pass_far(k)

    from_partner(near_half)
    for step in near_steps:
        q_arrived(step, 0, kv_heads)
    mine[3].wait()
    for h in range(kv_heads):
        add_up(h, near_row, block, [near_half], True, True)
        if h == 0:
            @pl.when(core == 0)
            def _():
                for k in near_steps[:-1]:
                    pass_far(k)

            pass_far(near_pieces - 1)
    from_partner(far_half)
    for h in range(kv_heads):
        add_up(h, near_row, block, [far_half], False, False)
        finish(h, near_row, block, acc[h])
    for h in range(kv_heads):
        def far(k):
            step = near_pieces + flip(1 - inner, k, near_pieces)
            q_arrived(step, h, 1)
            first_row = flip(home, step, pieces) * piece_rows
            add_up(h, first_row, piece_rows, [far_half, near_half], True, True)
            finish(h, first_row, piece_rows, acc[h, : per_kv * piece_rows])

        each(near_pieces, far)
    arrived(kv.at[ctx, :, : (n_head - 1) * rows], kv_sent)
    arrived(qbuf.at[: (n_head - 1) * rows], q_sent)
    if chips > 1:
        arrived(kv.at[: chips - 1], x_sent)
    arrived(kv.at[:chips], p_sent)


def shards(n_head, n_ctx, query, key, value, block_order):
    rows = query.shape[0]
    total = rows * n_head
    q_cols = query.shape[1] // n_head
    kv_cols = key.shape[1] // n_head
    kv_heads = kv_cols // HEAD_WIDTH
    per_kv = q_cols // kv_cols
    pair = 2
    pieces = n_head // pair
    hbm = pl.BlockSpec(memory_space=pltpu.HBM)
    dma = pltpu.SemaphoreType.DMA
    return pl.pallas_call(
        functools.partial(kernel, n_head, n_ctx, pair),
        out_shape=pltpu.VMEM((total, q_cols), jnp.bfloat16),
        in_specs=[hbm, hbm, hbm, hbm],
        out_specs=pl.BlockSpec(memory_space=pltpu.VMEM),
        scratch_shapes=[
            pltpu.VMEM((total, q_cols), jnp.bfloat16),
            pltpu.VMEM((n_ctx, 2, total, kv_cols), jnp.bfloat16),
            pltpu.VMEM((kv_heads, per_kv * total // 2, 2 * HEAD_WIDTH), jnp.float32),
            pltpu.SMEM(block_order.shape, jnp.int32),
            dma(()), dma(()), dma(()), dma(()),
            dma((kv_heads, pieces)), dma((n_head,)), dma((n_ctx // 2, n_head)), dma((n_ctx // 2, 2)), dma((3,)),
            pltpu.SemaphoreType.REGULAR((n_head,)), pltpu.SemaphoreType.REGULAR((n_ctx,)),
        ],
        compiler_params=pltpu.CompilerParams(
            collective_id=0, has_side_effects=True, vmem_limit_bytes=60 * 1024 * 1024
        ),
    )(block_order, query, key, value)


def solution(mesh):
    placed = (P(("ctx", "head"), None), P(("ctx", "head"), None), P(("ctx", "head"), None), P())
    return jax.shard_map(
        functools.partial(shards, mesh.shape["head"], mesh.shape["ctx"]),
        mesh=mesh, in_specs=placed, out_specs=P("ctx", "head"), check_vma=False,
    )
```

```python
import functools
import math

import jax
import jax.numpy as jnp
from jax import lax
from jax.experimental import pallas as pl
from jax.experimental.pallas import tpu as pltpu
from jax.sharding import PartitionSpec as P

HEAD_WIDTH = 128
MESH = pl.DeviceIdType.MESH
CAP = 50.0
IN_SCALE = 1.0 / (12.0 * CAP)
OUT_SCALE = CAP * math.log2(math.e)
HIDDEN = -4096.0


def flip(index, step, size):
    out, bit = 0, 1
    while bit < size:
        mine = (index // bit) % 2
        turn = (step // bit) % 2
        out = out + (mine + turn - 2 * mine * turn) * bit
        bit *= 2
    return out


def kernel(
    n_head, n_ctx, pair,
    block_order, query, key, value, out,
    qbuf, kv, acc, order,
    q_sent, kv_sent, x_sent, p_sent,
    q_recv, kv_recv, x_recv, p_recv, local_sem,
    head_ready, ctx_ready,
):
    me = lax.axis_index("head")
    ctx = lax.axis_index("ctx")
    chip, core = ctx // 2, ctx % 2
    partner = chip * 2 + 1 - core
    chips = n_ctx // 2
    pieces = n_head // pair
    rows = query.shape[0]
    total = rows * n_head
    block = total // 2
    q_cols = query.shape[1] // n_head
    kv_cols = key.shape[1] // n_head
    kv_heads = kv_cols // HEAD_WIDTH
    per_kv = q_cols // kv_cols
    h_cols = per_kv * HEAD_WIDTH
    piece_rows = rows * pair
    near_pieces = pieces // 2
    near = n_head // 2
    home = me // pair
    near_half = home // near_pieces
    far_half = 1 - near_half
    inner = (home + home // near_pieces) % 2
    same_core = [((chip + t) % chips) * 2 + core for t in range(chips)]
    other_core = [((chip + t) % chips) * 2 + 1 - core for t in range(chips)]
    peers = [flip(me, j, n_head) for j in range(1, n_head)]

    others = [("head", d) for d in peers] + [("ctx", c) for c in [partner] + same_core[1:]]
    at = {"head": me, "ctx": ctx}
    ready = {"head": head_ready, "ctx": ctx_ready}

    def tell(sem, axis, d):
        pl.semaphore_signal(sem, inc=1, device_id={axis: d}, device_id_type=MESH)

    def met(axis, d):
        @pl.when(d > at[axis])
        def _():
            pl.semaphore_wait(ready[axis].at[d], 1)

    barrier = pltpu.get_barrier_semaphore()
    for axis, d in others:
        @pl.when(d > at[axis])
        def _():
            tell(barrier, axis, d)

    def rows_of(s):
        return pl.ds(pl.multiple_of(s * rows, rows), rows)

    def cols_of(s, width):
        return pl.ds(pl.multiple_of(s * width, width), width)

    mine = [
        pltpu.make_async_copy(key.at[:, cols_of(me, kv_cols)], kv.at[ctx, 0, rows_of(me)], local_sem.at[0]),
        pltpu.make_async_copy(value.at[:, cols_of(me, kv_cols)], kv.at[ctx, 1, rows_of(me)], local_sem.at[0]),
        pltpu.make_async_copy(query.at[:, cols_of(me, q_cols)], qbuf.at[rows_of(me)], local_sem.at[1]),
    ]
    mine.append(pltpu.make_async_copy(block_order, order, local_sem.at[2]))
    for copy in mine:
        copy.start()

    @pl.when(me + chip + core > 0)
    def _():
        pl.semaphore_wait(barrier, me + chip + core)

    for axis, d in others:
        @pl.when(d < at[axis])
        def _():
            tell(ready[axis].at[at[axis]], axis, d)


    def kv_sends(d):
        return [
            pltpu.make_async_remote_copy(
                src_ref=src.at[:, cols_of(d, kv_cols)], dst_ref=kv.at[ctx, i, rows_of(me)],
                send_sem=kv_sent, recv_sem=kv_recv.at[me],
                device_id={"head": d}, device_id_type=MESH,
            )
            for i, src in enumerate((key, value))
        ]

    def q_send(d, h, heads):
        return pltpu.make_async_remote_copy(
            src_ref=query.at[:, pl.ds(pl.multiple_of(d * q_cols + h * h_cols, h_cols), heads * h_cols)],
            dst_ref=qbuf.at[rows_of(me), h * h_cols : (h + heads) * h_cols],
            send_sem=q_sent, recv_sem=q_recv.at[h, me // pair],
            device_id={"head": d}, device_id_type=MESH,
        )

    def arrived(ref, sem):
        pltpu.make_async_copy(ref, ref, sem).wait()

    def kv_ref(c, s):
        return kv.at[c, :, rows_of(s)]

    def pass_on(c, s, dest, send, recv):
        copy = pltpu.make_async_remote_copy(
            src_ref=kv_ref(c, s), dst_ref=kv_ref(c, s),
            send_sem=send, recv_sem=recv,
            device_id={"ctx": dest}, device_id_type=MESH,
        )
        copy.start()

    def to_partner(c, s):
        pass_on(c, s, partner, p_sent, p_recv.at[c // 2, s // near])

    def spread(j):
        s = flip(me, j, n_head)
        arrived(kv_ref(ctx, s), local_sem.at[0] if isinstance(j, int) and j == 0 else kv_recv.at[s])
        for c in same_core[1:]:
            pass_on(ctx, s, c, x_sent, x_recv.at[(chip - c // 2 + chips) % chips - 1, s])
        to_partner(ctx, s)

    def relay(j):
        s = flip(me, j, n_head)
        for c in same_core[1:]:
            arrived(kv_ref(c, s), x_recv.at[(c // 2 - chip + chips) % chips - 1, s])
            to_partner(c, s)

    def from_partner(half):
        for c in other_core:
            span = pl.ds(pl.multiple_of(half * block, block), block)
            arrived(kv.at[c, :, span], p_recv.at[c // 2, half])

    near_js, far_js = list(range(1, near)), list(range(near, n_head))

    def send_kv(js):
        for j in js:
            met("head", peers[j - 1])
            for copy in kv_sends(peers[j - 1]):
                copy.start()

    @pl.when(near_half == 1)
    def _():
        send_kv(far_js)

    for c in [partner] + same_core[1:]:
        met("ctx", c)
    spread(0)

    @pl.when(near_half == 1)
    def _():
        send_kv(near_js)

    @pl.when((near_half == 0) & (inner == 0))
    def _():
        send_kv(near_js[: pair - 1] + far_js[: near // 2] + near_js[pair - 1 :] + far_js[near // 2 :])

    @pl.when((near_half == 0) & (inner == 1))
    def _():
        send_kv(far_js[near // 2 :] + near_js + far_js[: near // 2])

    ordered = [far_half * near + i for i in range(near)]
    sends = [q_send(d, 0, kv_heads) for d in peers[: near - 1]]
    sends += [q_send(d, h, 1) for h in range(kv_heads) for d in ordered]
    for copy in sends:
        copy.start()

    ones = jnp.ones((2 * block, HEAD_WIDTH), jnp.bfloat16)

    def unit(h, first_row, m, half, t, diagonal):
        q_half = first_row // block
        q_block = order[2 * ctx + q_half]
        c0 = ((chip + t) % chips) * 2 + core
        c1 = ((chip + t) % chips) * 2 + 1 - core
        q_span = pl.ds(pl.multiple_of(first_row, piece_rows), m)
        k_span = pl.ds(pl.multiple_of(half * block, block), block)
        low = jnp.where(order[2 * c0 + half] <= q_block, 0.0, HIDDEN)
        high = jnp.where(order[2 * c1 + half] <= q_block, 0.0, HIDDEN)
        cols = slice(h * HEAD_WIDTH, (h + 1) * HEAD_WIDTH)
        q = jnp.concatenate(
            [qbuf[q_span, (h * per_kv + i) * HEAD_WIDTH : (h * per_kv + i + 1) * HEAD_WIDTH] for i in range(per_kv)],
            axis=0,
        )
        k = jnp.concatenate([kv[c0, 0, k_span, cols], kv[c1, 0, k_span, cols]], axis=0)
        v = jnp.concatenate([kv[c0, 1, k_span, cols], kv[c1, 1, k_span, cols]], axis=0)
        x = lax.dot_general(q, k, (((1,), (1,)), ((), ())), preferred_element_type=jnp.float32)
        x = jnp.tanh(x * IN_SCALE) * OUT_SCALE
        if diagonal:
            q_at = first_row - q_half * block + lax.broadcasted_iota(jnp.int32, (m, block), 0)
            visible = lax.broadcasted_iota(jnp.int32, (m, block), 1) <= q_at
            e = jnp.exp2(x[:, :block]).reshape(per_kv, m, block)
            left = jnp.where(visible[None], e, 0.0).reshape(per_kv * m, block)
        else:
            left = jnp.exp2(x[:, :block] + low)
        w = jnp.concatenate([left, jnp.exp2(x[:, block:] + high)], axis=1).astype(jnp.bfloat16)
        return jnp.dot(w, jnp.concatenate([v, ones], axis=1), preferred_element_type=jnp.float32)

    def q_arrived(step, h, heads):
        p = flip(home, step, pieces)
        count = pair
        first = p * pair
        if isinstance(step, int) and step == 0:
            mine[2].wait()
            first, count = flip(me, 1, n_head), pair - 1
        arrived(qbuf.at[pl.ds(pl.multiple_of(first * rows, rows), count * rows), h * h_cols : (h + heads) * h_cols], q_recv.at[h, p])

    def finish(h, first_row, m, a):
        span = pl.ds(pl.multiple_of(first_row, piece_rows), m)
        o = (a[:, :HEAD_WIDTH] / a[:, HEAD_WIDTH:]).astype(jnp.bfloat16)
        for i in range(per_kv):
            col = (h * per_kv + i) * HEAD_WIDTH
            out[span, col : col + HEAD_WIDTH] = o[i * m : (i + 1) * m]

    def each(count, body):
        lax.fori_loop(0, count, lambda i, carry: (body(i), carry)[1], 0)

    near_steps = range(near_pieces)
    far_steps = [near_pieces + flip(1 - inner, k, near_pieces) for k in near_steps]

    def far_peers(k):
        return [far_steps[k] * pair + t for t in range(pair)]

    near_row, far_row = near_half * block, far_half * block

    def add_up(h, first_row, m, halves, diagonal, start):
        a = acc.at[h, : per_kv * m]
        o = sum(unit(h, first_row, m, half, 0, diagonal and half is halves[0]) for half in halves)
        a[...] = o if start else a[...] + o

        def more(t):
            a[...] += sum(unit(h, first_row, m, half, t + 1, False) for half in halves)

        each(chips - 1, more)

    def pass_far(k):
        for j in far_peers(k):
            relay(j)

    later = (inner == 1) | ((near_half == 0) & (core == 0))

    for j in range(1, pair):
        spread(j)

    @pl.when(jnp.logical_not(later))
    def _():
        for j in range(pair, near):
            spread(j)

    for j in far_peers(0):
        spread(j)

    @pl.when(later)
    def _():
        for j in range(pair, near):
            spread(j)

    for k in near_steps[1:]:
        for j in far_peers(k):
            spread(j)
    for j in range(near):
        relay(j)

    @pl.when(core == 1)
    def _():
        for k in near_steps[:-1]:
            pass_far(k)

    from_partner(near_half)
    for step in near_steps:
        q_arrived(step, 0, kv_heads)
    mine[3].wait()
    for h in range(kv_heads):
        add_up(h, near_row, block, [near_half], True, True)
        if h == 0:
            @pl.when(core == 0)
            def _():
                for k in near_steps[:-1]:
                    pass_far(k)

            @pl.when(core == 1)
            def _():
                pass_far(near_pieces - 1)

    @pl.when(core == 0)
    def _():
        pass_far(near_pieces - 1)

    from_partner(far_half)
    for h in range(kv_heads):
        add_up(h, near_row, block, [far_half], False, False)
        finish(h, near_row, block, acc[h])
    for h in range(kv_heads):
        def far(k):
            step = near_pieces + flip(1 - inner, k, near_pieces)
            q_arrived(step, h, 1)
            first_row = flip(home, step, pieces) * piece_rows
            add_up(h, first_row, piece_rows, [far_half, near_half], True, True)
            finish(h, first_row, piece_rows, acc[h, : per_kv * piece_rows])

        each(near_pieces, far)
    arrived(kv.at[ctx, :, : (n_head - 1) * rows], kv_sent)
    arrived(qbuf.at[: (n_head - 1) * rows], q_sent)
    if chips > 1:
        arrived(kv.at[: chips - 1], x_sent)
    arrived(kv.at[:chips], p_sent)


def shards(n_head, n_ctx, query, key, value, block_order):
    rows = query.shape[0]
    total = rows * n_head
    q_cols = query.shape[1] // n_head
    kv_cols = key.shape[1] // n_head
    kv_heads = kv_cols // HEAD_WIDTH
    per_kv = q_cols // kv_cols
    pair = 2
    pieces = n_head // pair
    hbm = pl.BlockSpec(memory_space=pltpu.HBM)
    dma = pltpu.SemaphoreType.DMA
    return pl.pallas_call(
        functools.partial(kernel, n_head, n_ctx, pair),
        out_shape=pltpu.VMEM((total, q_cols), jnp.bfloat16),
        in_specs=[hbm, hbm, hbm, hbm],
        out_specs=pl.BlockSpec(memory_space=pltpu.VMEM),
        scratch_shapes=[
            pltpu.VMEM((total, q_cols), jnp.bfloat16),
            pltpu.VMEM((n_ctx, 2, total, kv_cols), jnp.bfloat16),
            pltpu.VMEM((kv_heads, per_kv * total // 2, 2 * HEAD_WIDTH), jnp.float32),
            pltpu.SMEM(block_order.shape, jnp.int32),
            dma(()), dma(()), dma(()), dma(()),
            dma((kv_heads, pieces)), dma((n_head,)), dma((max(n_ctx // 2 - 1, 1), n_head)), dma((n_ctx // 2, 2)), dma((3,)),
            pltpu.SemaphoreType.REGULAR((n_head,)), pltpu.SemaphoreType.REGULAR((n_ctx,)),
        ],
        compiler_params=pltpu.CompilerParams(
            collective_id=0, has_side_effects=True, vmem_limit_bytes=60 * 1024 * 1024
        ),
    )(block_order, query, key, value)


def solution(mesh):
    placed = (P(("ctx", "head"), None), P(("ctx", "head"), None), P(("ctx", "head"), None), P())
    return jax.shard_map(
        functools.partial(shards, mesh.shape["head"], mesh.shape["ctx"]),
        mesh=mesh, in_specs=placed, out_specs=P("ctx", "head"), check_vma=False,
    )
```
